32 devices in a mesh: tm: 4 (over y, x), space: 8 (over z, core).
Axes of the slice: x: 2, y: 2, z: 4, core: 2. Of those that a mesh axis runs over, the one named last changes fastest.
Arguments:
- thermal_field: float32 [128, 49152], P(('tm', 'space')), may hold values from 245 to 255
- seasonal_bucket: int32 [128], replicated, may hold values from 0 to 45, as said below
- season_of_record: int32 [128], replicated, may hold values from 0 to 7
Outputs:
- anomaly: float32 [128, 49152], P(('tm', 'space'))
The draws below stay inside these ranges and needn't reach their ends.
Inputs may be any that keep to these rules, and one draw needn't show every extreme that they name: `seasonal_bucket`: every group holds at least one day whose year is below 6.
All inputs are finite; a program needn't handle non-finite values.
Results may differ from the reference program's by a relative error of at most 0.0003.
Values sent between devices are 32-bit elements; how exact they have to be, the bound alone decides.
A program may use at most 64 MiB of HBM per device.

```python
import jax
import jax.numpy as jnp
from jax import lax

GROUPS = 46
YEARS = 8
BASE_YEARS = 6
TIME_STEPS = 128
MESH_POINTS = 49152


def calendar(key):
    ordering = jax.random.permutation(jax.random.fold_in(key, 11), TIME_STEPS)
    chosen_records = ordering[:GROUPS]
    random_group = jax.random.randint(jax.random.fold_in(key, 12), (TIME_STEPS,), 0, GROUPS)
    random_year = jax.random.randint(jax.random.fold_in(key, 13), (TIME_STEPS,), 0, YEARS)
    base_year = jax.random.randint(jax.random.fold_in(key, 14), (GROUPS,), 0, BASE_YEARS)
    groups = random_group.at[chosen_records].set(jnp.arange(GROUPS, dtype=jnp.int32))
    years = random_year.at[chosen_records].set(base_year)
    return (groups.astype(jnp.int32), years.astype(jnp.int32))


def draw_seasonal_bucket(key, part):
    return calendar(key)[0]


def draw_season_of_record(key, part):
    return calendar(key)[1]


def steps_of(rng, shape, pieces, least, high):
    def one(dim, blocks):
        steps = jax.random.uniform(jax.random.fold_in(jax.random.fold_in(rng, 6), dim), (blocks,), jnp.float32, least / len(pieces), high / len(pieces))
        return jnp.repeat(jnp.exp(steps), shape[dim] // blocks).reshape((-1,) + (1,) * (len(shape) - dim - 1))

    level = one(*pieces[0])
    for cut in pieces[1:]:
        level = level * one(*cut)
    return level


def setup_inputs(seed: int = 0) -> dict:
    splits = jax.random.split(jax.random.key(seed), 4)
    return {
        "thermal_field": jnp.clip(245.0 + 10.0 * jax.random.uniform(splits[0], (TIME_STEPS, MESH_POINTS), jnp.float32) ** steps_of(splits[0], (TIME_STEPS, MESH_POINTS), ((0, 32),), -0.2, 0.2), 245.0, 255.0),
        "seasonal_bucket": draw_seasonal_bucket(jax.random.fold_in(splits[3], 71), 0),
        "season_of_record": draw_season_of_record(jax.random.fold_in(splits[3], 71), 0),
    }


def reference(thermal_field, seasonal_bucket, season_of_record):
    group_ids = jnp.arange(GROUPS, dtype=jnp.int32)
    member = (seasonal_bucket[None, :] == group_ids[:, None]).astype(jnp.float32)
    reference_seasons = member * (season_of_record < BASE_YEARS).astype(jnp.float32)[None, :]
    counts = jnp.sum(reference_seasons, axis=1)
    bucket_aggregates = jnp.dot(reference_seasons, thermal_field, precision=lax.Precision.HIGHEST, preferred_element_type=jnp.float32)
    climate = bucket_aggregates / counts[:, None]
    chosen_records = jnp.dot(member.T, climate, precision=lax.Precision.HIGHEST, preferred_element_type=jnp.float32)
    return thermal_field - chosen_records
```

```python
import functools

import jax
import jax.numpy as jnp
from jax import lax
from jax.experimental import pallas as pl
from jax.experimental.pallas import tpu as pltpu
from jax.sharding import PartitionSpec as P

BASE_YEARS = 6
CHUNKS = 3


def for_peers(nt, ns, body):
    t, s = lax.axis_index("tm"), lax.axis_index("space")

    def one(dt, ds):
        pt, ps = lax.rem(t + dt, nt), lax.rem(s + ds, ns)
        body(pt, ps, pt * ns + ps)

    def step(i, carry):
        one(lax.rem(i, nt), 1 + lax.rem(i // nt + (ns // 2 - 1), ns - 1))
        return carry

    lax.fori_loop(0, nt * (ns - 1), step, 0)
    for dt in range(1, nt):
        one(dt, 0)


def kernel(nt, ns, chunks, x_hbm, bucket_ref, season_ref, out_ref,
           xv, recv, y, load_sem, own_sem, send1, recv1, send2, recv2):
    n = nt * ns
    rows, cells = x_hbm.shape
    mine = cells // n
    c = mine // chunks
    days = rows * n
    me = lax.axis_index("tm") * ns + lax.axis_index("space")

    load = pltpu.make_async_copy(x_hbm, xv, load_sem)
    load.start()
    own = []
    for k in range(chunks):
        own.append(pltpu.make_async_copy(
            x_hbm.at[:, pl.ds(pl.multiple_of(me * mine + k * c, 128), c)],
            recv.at[k, me], own_sem.at[k]))
        own[k].start()

    barrier = pltpu.get_barrier_semaphore()
    for_peers(nt, ns, lambda pt, ps, p: pl.semaphore_signal(
        barrier, inc=1, device_id=(pt, ps), device_id_type=pl.DeviceIdType.MESH))
    pl.semaphore_wait(barrier, n - 1)
    load.wait()

    for k in range(chunks):
        def push(pt, ps, p, k=k):
            pltpu.make_async_remote_copy(
                src_ref=xv.at[:, pl.ds(pl.multiple_of(p * mine + k * c, 128), c)],
                dst_ref=recv.at[k, me],
                send_sem=send1.at[k], recv_sem=recv1.at[k],
                device_id=(pt, ps), device_id_type=pl.DeviceIdType.MESH).start()
        for_peers(nt, ns, push)

    bucket = jnp.broadcast_to(bucket_ref[...], (days, days))
    season = jnp.broadcast_to(season_ref[...], (days, days))
    member = jnp.where((bucket == bucket.T) & (season < BASE_YEARS), 1.0, 0.0)
    inverse = 1.0 / jnp.sum(member, axis=1, keepdims=True)
    member = member.astype(jnp.bfloat16)

    def all_of(ref, sem):
        part = ref.at[pl.ds(0, n - 1)]
        pltpu.make_async_copy(part, part, sem).wait()

    for k in range(chunks):
        own[k].wait()
        all_of(recv.at[k], recv1.at[k])
        x = recv[k].reshape(days, c)
        high = x.astype(jnp.bfloat16)
        rest = x - high.astype(jnp.float32)
        middle = rest.astype(jnp.bfloat16)
        low = (rest - middle.astype(jnp.float32)).astype(jnp.bfloat16)
        total = jnp.dot(member, low, preferred_element_type=jnp.float32)
        total += jnp.dot(member, middle, preferred_element_type=jnp.float32)
        total += jnp.dot(member, high, preferred_element_type=jnp.float32)
        y[k] = (x - total * inverse).reshape(n, rows, c)

        def back(pt, ps, p, k=k):
            pltpu.make_async_remote_copy(
                src_ref=y.at[k, p],
                dst_ref=out_ref.at[:, pl.ds(pl.multiple_of(me * mine + k * c, 128), c)],
                send_sem=send2.at[k], recv_sem=recv2.at[k],
                device_id=(pt, ps), device_id_type=pl.DeviceIdType.MESH).start()
        for_peers(nt, ns, back)
        out_ref[:, pl.ds(pl.multiple_of(me * mine + k * c, 128), c)] = y[k, me]

    for k in range(chunks):
        all_of(recv.at[k], send1.at[k])
        all_of(recv.at[k], recv2.at[k])
        all_of(recv.at[k], send2.at[k])


def solution(mesh):
    nt, ns = mesh.shape["tm"], mesh.shape["space"]
    n = nt * ns

    def shards(thermal_field, seasonal_bucket, season_of_record):
        rows, cells = thermal_field.shape
        c = cells // n // CHUNKS
        vmem = pl.BlockSpec(memory_space=pltpu.VMEM)
        sems = pltpu.SemaphoreType.DMA
        return pl.pallas_call(
            functools.partial(kernel, nt, ns, CHUNKS),
            out_shape=jax.ShapeDtypeStruct((rows, cells), jnp.float32),
            in_specs=[pl.BlockSpec(memory_space=pl.ANY), vmem, vmem],
            out_specs=vmem,
            scratch_shapes=[
                pltpu.VMEM((rows, cells), jnp.float32),
                pltpu.VMEM((CHUNKS, n, rows, c), jnp.float32),
                pltpu.VMEM((CHUNKS, n, rows, c), jnp.float32),
                sems, sems((CHUNKS,)), sems((CHUNKS,)), sems((CHUNKS,)),
                sems((CHUNKS,)), sems((CHUNKS,)),
            ],
            compiler_params=pltpu.CompilerParams(collective_id=0, has_side_effects=True),
            name="anomaly",
        )(thermal_field, seasonal_bucket.reshape(1, -1), season_of_record.reshape(1, -1))

    placed = (P(("tm", "space"), None), P(), P())
    return jax.shard_map(
        shards, mesh=mesh, in_specs=placed, out_specs=P(("tm", "space"), None), check_vma=False
    )
```

```python
import functools

import jax
import jax.numpy as jnp
from jax import lax
from jax.experimental import pallas as pl
from jax.experimental.pallas import tpu as pltpu
from jax.sharding import PartitionSpec as P

BASE_YEARS = 6
CHUNKS = 3


def for_peers(nt, ns, body):
    t, s = lax.axis_index("tm"), lax.axis_index("space")

    def one(dt, ds):
        pt, ps = lax.rem(t + dt, nt), lax.rem(s + ds, ns)
        body(pt, ps, pt * ns + ps)

    def step(i, carry):
        one(lax.rem(i, nt), 1 + lax.rem(i // nt + (ns // 2 - 1), ns - 1))
        return carry

    lax.fori_loop(0, nt * (ns - 1), step, 0)
    for dt in range(1, nt):
        one(dt, 0)


def kernel(nt, ns, chunks, x_hbm, bucket_hbm, season_hbm, out_ref,
           calendar, date_sem, xv, recv, y, load_sem, own_sem, send1, recv1, send2, recv2):
    n = nt * ns
    rows, cells = x_hbm.shape
    mine = cells // n
    c = mine // chunks
    days = rows * n
    me = lax.axis_index("tm") * ns + lax.axis_index("space")

    load = pltpu.make_async_copy(x_hbm, xv, load_sem)
    load.start()
    dates = [pltpu.make_async_copy(ref, calendar.at[i], date_sem.at[i])
             for i, ref in enumerate((bucket_hbm, season_hbm))]
    for date in dates:
        date.start()
    own = []
    for k in range(chunks):
        own.append(pltpu.make_async_copy(
            x_hbm.at[:, pl.ds(pl.multiple_of(me * mine + k * c, 128), c)],
            recv.at[k, me], own_sem.at[k]))
        own[k].start()

    barrier = pltpu.get_barrier_semaphore()
    for_peers(nt, ns, lambda pt, ps, p: pl.semaphore_signal(
        barrier, inc=1, device_id=(pt, ps), device_id_type=pl.DeviceIdType.MESH))
    pl.semaphore_wait(barrier, n - 1)
    load.wait()

    for k in range(chunks):
        def push(pt, ps, p, k=k):
            pltpu.make_async_remote_copy(
                src_ref=xv.at[:, pl.ds(pl.multiple_of(p * mine + k * c, 128), c)],
                dst_ref=recv.at[k, me],
                send_sem=send1.at[k], recv_sem=recv1.at[k],
                device_id=(pt, ps), device_id_type=pl.DeviceIdType.MESH).start()
        for_peers(nt, ns, push)

    for date in dates:
        date.wait()
    bucket = jnp.broadcast_to(calendar[0], (days, days))
    season = jnp.broadcast_to(calendar[1], (days, days))
    member = jnp.where((bucket == bucket.T) & (season < BASE_YEARS), 1.0, 0.0)
    inverse = 1.0 / jnp.sum(member, axis=1, keepdims=True)
    member = member.astype(jnp.bfloat16)

    def all_of(ref, sem):
        part = ref.at[pl.ds(0, n - 1)]
        pltpu.make_async_copy(part, part, sem).wait()

    for k in range(chunks):
        own[k].wait()
        all_of(recv.at[k], recv1.at[k])
        x = recv[k].reshape(days, c)
        high = x.astype(jnp.bfloat16)
        rest = x - high.astype(jnp.float32)
        middle = rest.astype(jnp.bfloat16)
        low = (rest - middle.astype(jnp.float32)).astype(jnp.bfloat16)
        total = jnp.dot(member, low, preferred_element_type=jnp.float32)
        total += jnp.dot(member, middle, preferred_element_type=jnp.float32)
        total += jnp.dot(member, high, preferred_element_type=jnp.float32)
        y[k] = (x - total * inverse).reshape(n, rows, c)

        def back(pt, ps, p, k=k):
            pltpu.make_async_remote_copy(
                src_ref=y.at[k, p],
                dst_ref=out_ref.at[:, pl.ds(pl.multiple_of(me * mine + k * c, 128), c)],
                send_sem=send2.at[k], recv_sem=recv2.at[k],
                device_id=(pt, ps), device_id_type=pl.DeviceIdType.MESH).start()
        for_peers(nt, ns, back)
        out_ref[:, pl.ds(pl.multiple_of(me * mine + k * c, 128), c)] = y[k, me]

    for k in range(chunks):
        all_of(recv.at[k], send1.at[k])
        all_of(recv.at[k], recv2.at[k])
        all_of(recv.at[k], send2.at[k])


def solution(mesh):
    nt, ns = mesh.shape["tm"], mesh.shape["space"]
    n = nt * ns

    def shards(thermal_field, seasonal_bucket, season_of_record):
        rows, cells = thermal_field.shape
        c, days = cells // n // CHUNKS, rows * n
        vmem = pl.BlockSpec(memory_space=pltpu.VMEM)
        sems = pltpu.SemaphoreType.DMA
        return pl.pallas_call(
            functools.partial(kernel, nt, ns, CHUNKS),
            out_shape=jax.ShapeDtypeStruct((rows, cells), jnp.float32),
            in_specs=[pl.BlockSpec(memory_space=pltpu.HBM)] * 3,
            out_specs=vmem,
            scratch_shapes=[
                pltpu.VMEM((2, 1, days), jnp.int32), sems((2,)),
                pltpu.VMEM((rows, cells), jnp.float32),
                pltpu.VMEM((CHUNKS, n, rows, c), jnp.float32),
                pltpu.VMEM((CHUNKS, n, rows, c), jnp.float32),
                sems, sems((CHUNKS,)), sems((CHUNKS,)), sems((CHUNKS,)),
                sems((CHUNKS,)), sems((CHUNKS,)),
            ],
            compiler_params=pltpu.CompilerParams(collective_id=0, has_side_effects=True, vmem_limit_bytes=24 * 2**20),
            name="anomaly",
        )(*(pltpu.with_memory_space_constraint(a, pltpu.HBM) for a in (
            thermal_field, seasonal_bucket.reshape(1, -1), season_of_record.reshape(1, -1))))

    placed = (P(("tm", "space"), None), P(), P())
    return jax.shard_map(
        shards, mesh=mesh, in_specs=placed, out_specs=P(("tm", "space"), None), check_vma=False
    )
```

```python
import functools

import jax
import jax.numpy as jnp
from jax import lax
from jax.experimental import pallas as pl
from jax.experimental.pallas import tpu as pltpu
from jax.sharding import PartitionSpec as P

GROUPS = 46
BASE_YEARS = 6
CHUNKS = 8
LAG = 2
LEAD = 3
SHARE = 2
MESH = pl.DeviceIdType.MESH


def exact_dot(mask, x):
    high = x.astype(jnp.bfloat16)
    rest = x - high.astype(jnp.float32)
    middle = rest.astype(jnp.bfloat16)
    low = (rest - middle.astype(jnp.float32)).astype(jnp.bfloat16)
    total = jnp.dot(mask, low, preferred_element_type=jnp.float32)
    total += jnp.dot(mask, middle, preferred_element_type=jnp.float32)
    return total + jnp.dot(mask, high, preferred_element_type=jnp.float32)


def kernel(nt, ns, chunks, lag, lead, x_hbm, bucket_hbm, season_hbm, out_ref,
           calendar, date_sem, xv, recv, sums, other, y, load_sem,
           send1, recv1, send2, recv2, send3, recv3,
           got, done, send4, recv4, send5, recv5):
    nh, nq = ns // 2, ns // 4
    half, owners = nt * nh, nt * nq
    when = chunks - 1
    when_other = chunks // 2
    rows, cells = x_hbm.shape
    n = nt * ns
    direct = cells // SHARE // n
    start = direct * n
    mine = (cells - start) // owners
    c = mine // chunks
    days = rows * nt * ns
    t, s = lax.axis_index("tm"), lax.axis_index("space")
    h = s // nh
    local = s - h * nh
    first = nq * (1 - h)
    place = local - first
    is_owner = (place >= 0) & (place < nq)
    slot = t * nh + local
    partner = s + nq * (1 - 2 * h)

    load = pltpu.make_async_copy(x_hbm, xv, load_sem)
    load.start()
    dates = [pltpu.make_async_copy(ref, calendar.at[i], date_sem.at[i])
             for i, ref in enumerate((bucket_hbm, season_hbm))]
    for date in dates:
        date.start()

    def to_owners(body, others):
        for dq in range(nq):
            for dt in range(nt):
                if others and dt == dq == 0:
                    continue
                pt, pq = lax.rem(t + dt, nt), lax.rem(place + nq + dq, nq)
                body(pt, h * nh + first + pq, pt * nq + pq)

    def to_half(body):
        for dl in [(nh // 2 + i) % nh for i in range(nh)]:
            for dt in range(nt):
                if dt == dl == 0:
                    continue
                pt, at = lax.rem(t + dt, nt), lax.rem(local + dl, nh)
                body(pt, h * nh + at, pt * nh + at)

    barrier = pltpu.get_barrier_semaphore()

    def greet(pt, ps, p):
        pl.semaphore_signal(barrier, inc=1, device_id=(pt, ps), device_id_type=MESH)

    def to_all(body):
        for ds in [(nh + i) % ns for i in range(ns)]:
            for dt in range(nt):
                if dt == ds == 0:
                    continue
                pt, ps = lax.rem(t + dt, nt), lax.rem(s + ds, ns)
                body(pt, ps, pt * ns + ps)

    to_all(greet)
    pl.semaphore_wait(barrier, n - 1)
    who = t * ns + s
    own = pl.ds(pl.multiple_of(who * direct, 128), direct)

    def push(k, others):
        def one(pt, ps, p):
            pltpu.make_async_remote_copy(
                src_ref=xv.at[:, pl.ds(pl.multiple_of(start + p * mine + k * c, 128), c)],
                dst_ref=recv.at[k, slot], send_sem=send1.at[k], recv_sem=recv1.at[k],
                device_id=(pt, ps), device_id_type=MESH).start()
        to_owners(one, others)

    load.wait()

    def push_direct(pt, ps, p):
        pltpu.make_async_remote_copy(
            src_ref=xv.at[:, pl.ds(pl.multiple_of(p * direct, 128), direct)],
            dst_ref=got.at[who], send_sem=send4, recv_sem=recv4,
            device_id=(pt, ps), device_id_type=MESH).start()
    to_all(push_direct)
    got[who] = xv[:, own]
    for date in dates:
        date.wait()

    def all_direct(sem):
        part = got.at[pl.ds(0, n - 1)]
        pltpu.make_async_copy(part, part, sem).wait()

    def finish_direct():
        bucket = jnp.broadcast_to(calendar[0], (days, days))
        season = jnp.broadcast_to(calendar[1], (days, days))
        same = jnp.where((bucket == bucket.T) & (season < BASE_YEARS), 1.0, 0.0)
        inverse = 1.0 / jnp.sum(same, axis=1, keepdims=True)
        all_direct(recv4)
        x = got[...].reshape(days, direct)
        mean = exact_dot(same.astype(jnp.bfloat16), x) * inverse
        done[...] = (x - mean).reshape(n, rows, direct)

        def back_direct(pt, ps, p):
            pltpu.make_async_remote_copy(
                src_ref=done.at[p], dst_ref=out_ref.at[:, own],
                send_sem=send5, recv_sem=recv5,
                device_id=(pt, ps), device_id_type=MESH).start()
        to_all(back_direct)
        out_ref[:, own] = done[who]

    def all_of(count, sem):
        part = recv.at[0, pl.ds(0, count)]
        pltpu.make_async_copy(part, part, sem).wait()

    @pl.when(is_owner)
    def _():
        for k in range(min(lead, chunks)):
            push(k, True)
        me = t * nq + place
        base = pl.multiple_of(start + me * mine, 128)
        padded = sums.shape[1]

        bucket, season = calendar[0], calendar[1]
        key = jnp.where(season < BASE_YEARS, bucket, -1)
        width = nh * rows
        here = half * rows
        order = lax.broadcasted_iota(jnp.int32, (here, days), 0)
        day = (order // width) * (2 * width) + h * width + lax.rem(order, width)
        pick = day == lax.broadcasted_iota(jnp.int32, (here, days), 1)

        def of_half(row):
            return jnp.sum(jnp.where(pick, row, 0), axis=1, keepdims=True)

        member = of_half(bucket) == lax.broadcasted_iota(jnp.int32, (here, padded), 1)
        member = jnp.where(member, 1.0, 0.0).astype(jnp.bfloat16)
        key_row = jnp.broadcast_to(of_half(key), (here, here)).T[:1]
        group = lax.broadcasted_iota(jnp.int32, (padded, here), 0)
        baseline = jnp.where(group == key_row, 1.0, 0.0).astype(jnp.bfloat16)
        counted = lax.broadcasted_iota(jnp.int32, (padded, days), 0) == key
        counts = jnp.sum(jnp.where(counted, 1.0, 0.0), axis=1, keepdims=True)
        inverse = 1.0 / jnp.maximum(counts, 1.0)

        def swap(k):
            return pltpu.make_async_remote_copy(
                src_ref=sums.at[k], dst_ref=other.at[k],
                send_sem=send2.at[k], recv_sem=recv2.at[k],
                device_id=(t, partner), device_id_type=MESH)

        def finish(k):
            swap(k).wait_recv()
            climate = (sums[k] + other[k]) * inverse
            x = recv[k].reshape(here, c)
            y[k] = (x - exact_dot(member, climate)).reshape(half, rows, c)
            at = pl.ds(pl.multiple_of(base + k * c, 128), c)

            def back(pt, ps, p):
                pltpu.make_async_remote_copy(
                    src_ref=y.at[k, p], dst_ref=out_ref.at[:, at],
                    send_sem=send3.at[k], recv_sem=recv3.at[k],
                    device_id=(pt, ps), device_id_type=MESH).start()
            to_half(back)
            out_ref[:, at] = y[k, slot]

        for k in range(chunks):
            if k + lead < chunks:
                push(k + lead, True)
            recv[k, slot] = xv[:, pl.ds(pl.multiple_of(base + k * c, 128), c)]
            all_of(half - 1, recv1.at[k])
            sums[k] = exact_dot(baseline, recv[k].reshape(here, c))
            swap(k).start()
            if k == when:
                finish_direct()
            if k >= lag:
                finish(k - lag)
        for k in range(max(chunks - lag, 0), chunks):
            finish(k)

        for k in range(chunks):
            all_of(owners - 1, send1.at[k])
            swap(k).wait_send()
            all_of(owners - 1, recv3.at[k])
            all_of(half - 1, send3.at[k])

    @pl.when(jnp.logical_not(is_owner))
    def _():
        for k in range(chunks):
            push(k, False)
        for k in range(chunks):
            all_of(owners, send1.at[k])
            if k == when_other:
                finish_direct()
            all_of(owners, recv3.at[k])

    all_direct(send4)
    all_direct(recv5)
    all_direct(send5)


def solution(mesh):
    nt, ns = mesh.shape["tm"], mesh.shape["space"]
    half, owners = nt * (ns // 2), nt * (ns // 4)

    def shards(thermal_field, seasonal_bucket, season_of_record):
        rows, cells = thermal_field.shape
        n = nt * ns
        direct = cells // SHARE // n
        c, days = (cells - direct * n) // owners // CHUNKS, rows * n
        sems = pltpu.SemaphoreType.DMA
        per_chunk = sems((CHUNKS,))
        vmem = functools.partial(pltpu.VMEM, dtype=jnp.float32)
        return pl.pallas_call(
            functools.partial(kernel, nt, ns, CHUNKS, LAG, LEAD),
            out_shape=jax.ShapeDtypeStruct((rows, cells), jnp.float32),
            in_specs=[pl.BlockSpec(memory_space=pltpu.HBM)] * 3,
            out_specs=pl.BlockSpec(memory_space=pltpu.VMEM),
            scratch_shapes=[
                pltpu.VMEM((2, 1, days), jnp.int32), sems((2,)),
                vmem((rows, cells)),
                vmem((CHUNKS, half, rows, c)),
                vmem((CHUNKS, GROUPS, c)),
                vmem((CHUNKS, GROUPS, c)),
                vmem((CHUNKS, half, rows, c)),
                sems, per_chunk, per_chunk, per_chunk, per_chunk,
                per_chunk, per_chunk,
                vmem((n, rows, direct)), vmem((n, rows, direct)),
                sems, sems, sems, sems,
            ],
            compiler_params=pltpu.CompilerParams(
                collective_id=0, has_side_effects=True, vmem_limit_bytes=36 * 2**20),
            name="anomaly",
        )(*(pltpu.with_memory_space_constraint(a, pltpu.HBM) for a in (
            thermal_field, seasonal_bucket.reshape(1, -1), season_of_record.reshape(1, -1))))

    placed = (P(("tm", "space"), None), P(), P())
    return jax.shard_map(
        shards, mesh=mesh, in_specs=placed, out_specs=P(("tm", "space"), None), check_vma=False
    )
```
